256 devices in a mesh: seq: 64 (over z, x, core), head: 4 (over y).
Axes of the slice: x: 4, y: 4, z: 8, core: 2. Of those that a mesh axis runs over, the one named last changes fastest.
Arguments:
- queries: bfloat16 [65536, 2048], P('seq', 'head'), may hold values from -200 to 200
- keys: bfloat16 [65536, 2048], P('seq', 'head'), may hold values from -6 to 6
- values: bfloat16 [65536, 2048], P('seq', 'head'), may hold values from -12 to 12
- gate_bias: float32 [16], P('head'), may hold values from -2 to 2
- out_weight: bfloat16 [2048, 4096], P(None, 'head'), may hold values from -0.125 to 0.125
Outputs:
- layer_out: bfloat16 [65536, 4096], P('seq', 'head')
The draws below stay inside these ranges and needn't reach their ends.
All inputs are finite; a program needn't handle non-finite values.
Results may differ from the reference program's by a relative error of at most 0.007.
Values may be sent and summed in bfloat16 or wider, within the bound.
No kernel may reach another device: no remote copies, remote signals or barrier semaphores. Data moves between devices by JAX's collectives and lax.ppermute only.
A program may use at most 128 MiB of HBM per device.

```python
import jax
import jax.numpy as jnp
from jax import lax

D = 4096
HEADS = 16
DH = 128
SEG = 256
TOKENS = 65536


def sign_field(key, salt, shape):
    flips = jax.random.bernoulli(jax.random.fold_in(key, salt), 0.5, shape)
    return jnp.where(flips, 1.0, -1.0).astype(jnp.float32)


def column_pattern(key):
    per_segment = sign_field(key, 21, (TOKENS // SEG, HEADS * DH))
    return jnp.repeat(per_segment, SEG, axis=0)


def key_signs(key):
    rates = jax.random.uniform(jax.random.fold_in(key, 24), (TOKENS // SEG, HEADS), jnp.float32, 0.2, 0.8)
    coins = jax.random.uniform(jax.random.fold_in(key, 22), (TOKENS, HEADS), jnp.float32)
    signs = jnp.where(coins < jnp.repeat(rates, SEG, axis=0), 1.0, -1.0).astype(jnp.float32)
    return jnp.repeat(signs, DH, axis=1)


def query_signs(key):
    return jnp.repeat(sign_field(key, 23, (TOKENS, HEADS)), DH, axis=1)


def position_shift():
    positions = jnp.arange(TOKENS).astype(jnp.float32)
    return -1.5 + 3.0 * (positions + 0.5) / TOKENS


def key_table(key):
    noise = jax.random.normal(jax.random.fold_in(key, 11), (TOKENS, HEADS * DH), jnp.float32)
    table = noise + 2.0 * key_signs(key) * column_pattern(key) + position_shift()[:, None]
    return jnp.clip(table, -6.0, 6.0)


def draw_keys(key, part):
    return key_table(key).astype(jnp.bfloat16)


def draw_queries(key, part):
    base_draw = jax.random.normal(jax.random.fold_in(key, 12), (TOKENS, HEADS * DH), jnp.float32)
    base_draw = base_draw + 0.75 * query_signs(key) * column_pattern(key)
    return jnp.clip(base_draw, -200.0, 200.0).astype(jnp.bfloat16)


def draw_values(key, part):
    noise = jax.random.normal(jax.random.fold_in(key, 13), (TOKENS, HEADS * DH), jnp.float32)
    column_off = jax.random.normal(jax.random.fold_in(key, 14), (HEADS * DH,), jnp.float32)
    segment_off = jax.random.normal(jax.random.fold_in(key, 15), (TOKENS // SEG, HEADS * DH), jnp.float32)
    linked = jax.random.normal(jax.random.fold_in(key, 16), (TOKENS // SEG, HEADS * DH), jnp.float32)
    table = noise + column_off[None, :] + jnp.repeat(segment_off, SEG, axis=0)
    table = table + 1.5 * key_signs(key) * jnp.repeat(linked, SEG, axis=0)
    return jnp.clip(table, -12.0, 12.0).astype(jnp.bfloat16)


def shard_levels(stream_key, shape, split, least, top_value):
    gain = 1.0
    for dim, parts in split:
        heights = jax.random.uniform(jax.random.fold_in(jax.random.fold_in(stream_key, 6), dim), (parts,), jnp.float32, least / len(split), top_value / len(split))
        gain = gain * jnp.repeat(jnp.exp(heights), shape[dim] // parts).reshape((-1,) + (1,) * (len(shape) - 1 - dim))
    return gain


def scatter_about(own_key, dims, spread, bound, pieces=(), held_as=jnp.bfloat16):
    array = spread * jax.random.normal(own_key, dims, jnp.float32)
    if pieces:
        array = array * shard_levels(own_key, dims, pieces, -0.22, 0.18)
    return jnp.clip(array, -bound, bound).astype(held_as)


def setup_inputs(seed: int = 0) -> dict:
    key_list = jax.random.split(jax.random.key(seed), 6)
    return {
        "queries": draw_queries(jax.random.fold_in(key_list[5], 71), 0),
        "keys": draw_keys(jax.random.fold_in(key_list[5], 71), 0),
        "values": draw_values(jax.random.fold_in(key_list[5], 71), 0),
        "gate_bias": jnp.clip(jax.random.uniform(key_list[3], (HEADS,), jnp.float32, -2.0, 2.0) * shard_levels(key_list[3], (HEADS,), ((0, 4),), -0.4, 0.0), -2.0, 2.0),
        "out_weight": scatter_about(key_list[4], (HEADS * DH, D), (HEADS * DH) ** -0.5, 0.125, ((1, 4),)),
    }


def reference(queries, keys, values, gate_bias, out_weight):
    seg_count = TOKENS // SEG
    blk_shape = (seg_count, SEG, HEADS, DH)
    query_blk = queries.reshape(blk_shape)
    key_blk = keys.reshape(blk_shape)
    value_blk = values.reshape(blk_shape)
    gate_open = jax.nn.sigmoid(gate_bias.astype(jnp.float32))
    positions = jnp.arange(SEG)
    causal = positions[:, None] >= positions[None, :]
    score_scale = 1.0 / (DH ** 0.5)
    high = lax.Precision.HIGHEST

    def segment(state_pair, inputs_seg):
        memory, normalizer = state_pair
        query_seg, key_seg, value_seg = inputs_seg
        query_flt = query_seg.astype(jnp.float32)
        key_flt = key_seg.astype(jnp.float32)
        value_flt = value_seg.astype(jnp.float32)
        query_map = jax.nn.elu(query_flt) + 1.0
        key_map = (jax.nn.elu(key_flt) + 1.0).astype(jnp.bfloat16).astype(jnp.float32)
        recall = jnp.einsum('thd,hde->the', query_map, memory, precision=high)
        denominator = jnp.einsum('thd,hd->th', query_map, normalizer, precision=high) + 1.0
        recall = recall / denominator[:, :, None]
        scores = jnp.einsum('qhd,khd->hqk', query_flt, key_flt, precision=high) * score_scale
        scores = jnp.where(causal[None], scores, jnp.float32(-1e30))
        weights = jax.nn.softmax(scores, axis=-1).astype(jnp.bfloat16).astype(jnp.float32)
        local_out = jnp.einsum('hqk,khd->qhd', weights, value_flt, precision=high)
        mixed = gate_open[None, :, None] * recall + (1.0 - gate_open)[None, :, None] * local_out
        context = mixed.astype(jnp.bfloat16).reshape(SEG, HEADS * DH)
        projected = jnp.dot(context, out_weight, preferred_element_type=jnp.float32).astype(jnp.bfloat16)
        memory = memory + jnp.einsum('thd,the->hde', key_map, value_flt, precision=high)
        normalizer = normalizer + jnp.sum(key_map, axis=0)
        return (memory, normalizer), projected

    start_state = (jnp.zeros((HEADS, DH, DH), jnp.float32), jnp.zeros((HEADS, DH), jnp.float32))
    ignored, outputs = lax.scan(segment, start_state, (query_blk, key_blk, value_blk))
    return outputs.reshape(TOKENS, D)
```

```python
import jax
import jax.numpy as jnp
from jax import lax
from jax.experimental import pallas as pl
from jax.experimental.pallas import tpu as pltpu
from jax.sharding import Mesh
from jax.sharding import PartitionSpec as P

DH = 128
SEG = 256
SEQ = ("seq_0", "seq_1", "seq_2")
BF = jnp.bfloat16
F32 = jnp.float32
ROWS = DH + 8


def feature(x):
    x = x.astype(F32)
    return jnp.where(x > 0.0, x + 1.0, jnp.exp(jnp.minimum(x, 0.0)))


def state_kernel(k_ref, v_ref, total_ref, inner_ref, norm_ref):
    segs = k_ref.shape[0] // SEG
    heads = k_ref.shape[1] // DH
    first = pl.program_id(0) * heads
    for h in range(heads):
        cols = slice(h * DH, (h + 1) * DH)
        mem = jnp.zeros((DH, DH), F32)
        norm = jnp.zeros((ROWS - DH, DH), F32)
        for s in range(segs):
            rows = slice(s * SEG, (s + 1) * SEG)
            if s > 0:
                inner_ref[s - 1, first + h] = mem
            norm_ref[first + h, s : s + 1, :] = norm[:1]
            key_map = feature(k_ref[rows, cols]).astype(BF)
            mem = mem + lax.dot_general(
                key_map, v_ref[rows, cols], (((0,), (0,)), ((), ())), preferred_element_type=F32
            )
            norm = norm + jnp.dot(jnp.ones((ROWS - DH, SEG), BF), key_map, preferred_element_type=F32)
        total_ref[first + h, :DH, :] = mem
        total_ref[first + h, DH:, :] = norm


def local_kernel(gate_ref, q_ref, k_ref, v_ref, out_ref):
    heads = q_ref.shape[1] // DH
    scale = 1.0 / DH**0.5 * 1.4426950408889634
    for s in range(q_ref.shape[0] // SEG):
        rows = slice(s * SEG, (s + 1) * SEG)
        for h in range(heads):
            cols = slice(h * DH, (h + 1) * DH)
            rest = 1.0 - gate_ref[h]
            scores = lax.dot_general(
                q_ref[rows, cols], k_ref[rows, cols], (((1,), (1,)), ((), ())), preferred_element_type=F32
            )
            row_at = lax.broadcasted_iota(jnp.int32, (SEG, SEG), 0)
            col_at = lax.broadcasted_iota(jnp.int32, (SEG, SEG), 1)
            scores = jnp.where(row_at >= col_at, scores * scale, -1e30)
            weights = jnp.exp2(scores - jnp.max(scores, axis=1, keepdims=True)).astype(BF)
            wide = jnp.concatenate([v_ref[rows, cols], jnp.ones((SEG, DH), BF)], axis=1)
            out = jnp.dot(weights, wide, preferred_element_type=F32)
            out_ref[rows, cols] = (out[:, :DH] * (rest / out[:, DH:])).astype(out_ref.dtype)


def context_kernel(first, gate_ref, q_ref, local_ref, before_ref, inner_ref, norm_ref, out_ref):
    heads = q_ref.shape[1] // DH
    for i in range(out_ref.shape[0] // SEG):
        s = first + i
        rows = slice(s * SEG, (s + 1) * SEG)
        outs = slice(i * SEG, (i + 1) * SEG)
        for h in range(heads):
            cols = slice(h * DH, (h + 1) * DH)
            query_map = feature(q_ref[rows, cols]).astype(BF)
            mem = before_ref[h, :DH, :]
            norm = before_ref[h, DH : DH + 1, :] + norm_ref[h, s : s + 1, :]
            if s > 0:
                mem = mem + inner_ref[s - 1, h]
            norm = jnp.broadcast_to(norm.astype(BF), (DH, DH))
            top = jnp.dot(query_map, mem.astype(BF), preferred_element_type=F32)
            bottom = lax.dot_general(query_map, norm, (((1,), (1,)), ((), ())), preferred_element_type=F32)
            recall = gate_ref[h] * top / (bottom + 1.0)
            out_ref[outs, cols] = (recall + local_ref[rows, cols].astype(F32)).astype(BF)


def project_kernel(near, far, at_ref, *refs):
    own_ref, prev_ref, next_ref, far_a_ref, far_b_ref, w_ref, sum_ref = refs[:7]
    out_ref = refs[-1]
    rows, tile = out_ref.shape
    col = pl.multiple_of(pl.program_id(0) * tile, tile)
    width = own_ref.shape[1]
    groups = w_ref.shape[0] // width
    half = rows // 2

    def part(offset):
        start = pl.multiple_of(lax.rem(at_ref[0] + offset, groups) * width, width)
        return w_ref[pl.ds(start, width), pl.ds(col, tile)]

    if near:
        acc = jnp.dot(own_ref[...], part(0), preferred_element_type=F32)
        acc = acc + jnp.dot(prev_ref[...], part(groups - 1), preferred_element_type=F32)
        acc = acc + jnp.dot(next_ref[...], part(1), preferred_element_type=F32)
    else:
        acc = sum_ref[:, pl.ds(col, tile)]
    if far:
        weight = part(2)
        top = acc[:half] + jnp.dot(far_a_ref[...], weight, preferred_element_type=F32)
        bottom = acc[half:] + jnp.dot(far_b_ref[...], weight, preferred_element_type=F32)
        out_ref[:half, :] = top.astype(out_ref.dtype)
        out_ref[half:, :] = bottom.astype(out_ref.dtype)
    else:
        out_ref[...] = acc


VMEM_SPEC = pl.BlockSpec(memory_space=pltpu.VMEM)
SMEM_SPEC = pl.BlockSpec(memory_space=pltpu.SMEM)


def near_core(x):
    return pltpu.with_memory_space_constraint(x, pltpu.VMEM)


def params(mib):
    return pltpu.CompilerParams(vmem_limit_bytes=mib * 2**20)


def state_call(keys, values):
    heads = keys.shape[1] // DH
    segs = keys.shape[0] // SEG
    block = pl.BlockSpec((keys.shape[0], 2 * DH), lambda i: (0, i))
    return pl.pallas_call(
        state_kernel,
        grid=(heads // 2,),
        in_specs=[block, block],
        out_specs=(VMEM_SPEC,) * 3,
        out_shape=(
            pltpu.VMEM((heads, ROWS, DH), F32),
            pltpu.VMEM((segs - 1, heads, DH, DH), F32),
            pltpu.VMEM((heads, 8, DH), F32),
        ),
        compiler_params=params(12),
        name="state",
    )(keys, values)


def local_call(gate, q, k, v):
    n, width = q.shape
    return pl.pallas_call(
        local_kernel,
        in_specs=[SMEM_SPEC] + [VMEM_SPEC] * 3,
        out_specs=VMEM_SPEC,
        out_shape=pltpu.VMEM((n, width), BF),
        compiler_params=params(12),
        cost_estimate=pl.CostEstimate(
            flops=4 * n * SEG * width, transcendentals=n * SEG * 4, bytes_accessed=8 * n * width
        ),
        name="local",
    )(gate, q, k, v)


def context_call(first, count, gate, q, local, before, inner, norm):
    return pl.pallas_call(
        lambda *refs: context_kernel(first, *refs),
        in_specs=[SMEM_SPEC] + [VMEM_SPEC] * 5,
        out_specs=VMEM_SPEC,
        out_shape=pltpu.VMEM((count * SEG, q.shape[1]), BF),
        compiler_params=params(12),
    )(gate, q, local, near_core(before), inner, norm)


def project_call(at, pieces, weight, total_rows, chunk, near, far, partial, so_far):
    n = weight.shape[1]
    tile = n // 4
    rows = pieces[0].shape[0]
    if partial is None:
        partial = at
    kept = [pieces[0]] * 5
    for i, piece in enumerate(pieces):
        if piece is not None:
            kept[i] = piece
    operands = [at, *map(near_core, kept), weight, partial]
    specs = [SMEM_SPEC] + [VMEM_SPEC] * 6 + [SMEM_SPEC if partial is at else VMEM_SPEC]
    aliases = {}
    if so_far is not None:
        aliases = {len(operands): 0}
        operands.append(so_far)
        specs.append(pl.BlockSpec(memory_space=pl.ANY))
    if far:
        out_shape = jax.ShapeDtypeStruct((total_rows, n), BF)
        out_spec = pl.BlockSpec((rows, tile), lambda j: (chunk, j))
    else:
        out_shape = jax.ShapeDtypeStruct((rows, n), F32)
        out_spec = pl.BlockSpec((rows, tile), lambda j: (0, j))
    width = (3 * near + far) * weight.shape[0] // 4
    return pl.pallas_call(
        lambda *refs: project_kernel(near, far, *refs),
        grid=(n // tile,),
        in_specs=specs,
        out_specs=out_spec,
        out_shape=out_shape,
        input_output_aliases=aliases,
        compiler_params=params(12),
        cost_estimate=pl.CostEstimate(flops=2 * rows * width * n, transcendentals=0, bytes_accessed=2 * width * n),
    )(*operands)


def turn(value, axis, step):
    size = lax.axis_size(axis)
    return lax.ppermute(value, axis, [(i, (i + step) % size) for i in range(size)])


def states_before(total):
    heads = total.shape[0]
    halves = total.reshape(2, heads // 2 * ROWS, DH)
    core = lax.axis_index("seq_2")
    mine = lax.dynamic_index_in_dim(halves, core, 0, keepdims=False)
    theirs = lax.dynamic_index_in_dim(halves, 1 - core, 0, keepdims=False)
    got = turn(theirs.astype(BF), "seq_2", 1).astype(F32)
    chip = mine + got
    sent = chip.astype(BF)
    x = lax.axis_index("seq_1")
    size = lax.axis_size("seq_1")
    plane, before = chip, jnp.zeros_like(chip)
    for k in range(1, size):
        piece = turn(sent, "seq_1", k).astype(F32)
        plane = plane + piece
        before = before + jnp.where(x >= k, piece, 0.0)
    z = lax.axis_index("seq_0")
    size = lax.axis_size("seq_0")
    beside = lax.ppermute(plane.astype(BF), "seq_0", [(i, i ^ 1) for i in range(size)]).astype(F32)
    before = before + jnp.where(z % 2 == 1, beside, 0.0)
    pair = (plane + beside).astype(BF)
    for k in range(2, size, 2):
        piece = turn(pair, "seq_0", k)
        before = before + jnp.where(z >= k, piece.astype(F32), 0.0)
    first = core == 0
    swapped = turn(jnp.where(first, before + mine, before).astype(BF), "seq_2", 1).astype(F32)
    own = jnp.where(first, before, before + got)
    low = jnp.where(first, own, swapped)
    high = jnp.where(first, swapped, own)
    return jnp.concatenate([low, high], axis=0).reshape(heads, ROWS, DH)


def layer(queries, keys, values, gate_bias, out_weight):
    rows = queries.shape[0]
    segs = rows // SEG
    chunks = 2
    gate = jax.nn.sigmoid(gate_bias)
    at = jnp.full((1,), lax.axis_index("head"), jnp.int32)
    total, inner, norm = state_call(keys, values)
    before = states_before(total)
    near_q = near_core(queries)
    local = local_call(gate, near_q, near_core(keys), near_core(values))
    weight = near_core(out_weight)
    pieces = []
    for c in range(chunks):
        own = context_call(c * segs // chunks, segs // chunks, gate, near_q, local, before, inner, norm)
        half = own.shape[0] // 2
        prev = turn(own, "head", 1)
        nxt = turn(own, "head", -1)
        far_a = turn(prev[:half], "head", 1)
        far_b = turn(nxt[half:], "head", -1)
        pieces.append((own, prev, nxt, far_a, far_b))
    partial = project_call(at, (*pieces[1][:3], None, None), weight, rows, 1, True, False, None, None)
    out = project_call(at, pieces[0], weight, rows, 0, True, True, None, None)
    own, _, _, far_a, far_b = pieces[1]
    out = project_call(at, (own, None, None, far_a, far_b), weight, rows, 1, False, True, near_core(partial), out)
    return out


def solution(mesh):
    finer = Mesh(
        mesh.devices.reshape(8, 4, 2, mesh.shape["head"]), ("seq_0", "seq_1", "seq_2", "head")
    )
    placed = (P(SEQ, "head"), P(SEQ, "head"), P(SEQ, "head"), P("head"), P(None, "head"))
    return jax.shard_map(layer, mesh=finer, in_specs=placed, out_specs=P(SEQ, "head"), check_vma=False)
```

```python
import jax
import jax.numpy as jnp
from jax import lax
from jax.experimental import pallas as pl
from jax.experimental.pallas import tpu as pltpu
from jax.sharding import Mesh
from jax.sharding import PartitionSpec as P

DH = 128
SEG = 256
SEQ = ("seq_0", "seq_1", "seq_2")
BF = jnp.bfloat16
F32 = jnp.float32
ROWS = DH + 8


def feature(x):
    x = x.astype(F32)
    return jnp.where(x > 0.0, x + 1.0, jnp.exp(jnp.minimum(x, 0.0)))


def fetch(sources, targets, sems):
    segs = targets[0].shape[0] // SEG
    copies = []
    for s in range(segs):
        rows = pl.ds(s * SEG, SEG)
        group = []
        for i, (source, target) in enumerate(zip(sources, targets)):
            copy = pltpu.make_async_copy(source.at[rows], target.at[rows], sems.at[s * len(sources) + i])
            copy.start()
            group.append(copy)
        copies.append(group)
    return copies


def state_kernel(k_hbm, v_hbm, total_ref, inner_ref, norm_ref, k_ref, v_ref, sems):
    segs = k_ref.shape[0] // SEG
    heads = k_ref.shape[1] // DH
    copies = fetch((k_hbm, v_hbm), (k_ref, v_ref), sems)
    norms = [jnp.zeros((ROWS - DH, DH), F32)] * heads
    for s in range(segs):
        rows = slice(s * SEG, (s + 1) * SEG)
        for copy in copies[s]:
            copy.wait()
        for h in range(heads):
            cols = slice(h * DH, (h + 1) * DH)
            norm_ref[h, s : s + 1, :] = norms[h][:1]
            key_map = feature(k_ref[rows, cols]).astype(BF)
            mem = lax.dot_general(
                key_map, v_ref[rows, cols], (((0,), (0,)), ((), ())), preferred_element_type=F32
            )
            if s > 0:
                mem = mem + inner_ref[s - 1, h]
            norms[h] = norms[h] + jnp.dot(jnp.ones((ROWS - DH, SEG), BF), key_map, preferred_element_type=F32)
            if s < segs - 1:
                inner_ref[s, h] = mem
            else:
                total_ref[h, :DH, :] = mem
                total_ref[h, DH:, :] = norms[h]


def local_kernel(gate_ref, q_hbm, k_hbm, v_hbm, out_ref, q_ref, k_ref, v_ref, sems):
    heads = q_ref.shape[1] // DH
    scale = 1.0 / DH**0.5 * 1.4426950408889634
    copies = fetch((q_hbm, k_hbm, v_hbm), (q_ref, k_ref, v_ref), sems)
    for s in range(q_ref.shape[0] // SEG):
        rows = slice(s * SEG, (s + 1) * SEG)
        for copy in copies[s]:
            copy.wait()
        for h in range(heads):
            cols = slice(h * DH, (h + 1) * DH)
            rest = 1.0 - gate_ref[h : h + 1, :]
            scores = lax.dot_general(
                q_ref[rows, cols], k_ref[rows, cols], (((1,), (1,)), ((), ())), preferred_element_type=F32
            )
            row_at = lax.broadcasted_iota(jnp.int32, (SEG, SEG), 0)
            col_at = lax.broadcasted_iota(jnp.int32, (SEG, SEG), 1)
            scores = jnp.where(row_at >= col_at, scores * scale, -1e30)
            weights = jnp.exp2(scores - jnp.max(scores, axis=1, keepdims=True)).astype(BF)
            wide = jnp.concatenate([v_ref[rows, cols], jnp.ones((SEG, DH), BF)], axis=1)
            out = jnp.dot(weights, wide, preferred_element_type=F32)
            out_ref[rows, cols] = (out[:, :DH] * (rest / out[:, DH:])).astype(out_ref.dtype)


def context_kernel(first, gate_ref, q_ref, local_ref, own_ref, swapped_ref, inner_ref, norm_ref, out_ref):
    heads = q_ref.shape[1] // DH
    front = gate_ref[heads : heads + 1, :] == 0.0
    for h in range(heads):
        cols = slice(h * DH, (h + 1) * DH)
        low = h < heads // 2
        part = slice(h % (heads // 2) * ROWS, h % (heads // 2) * ROWS + DH + 1)
        own, swapped = own_ref[part, :], swapped_ref[part, :].astype(F32)
        before = jnp.where(front, own, swapped) if low else jnp.where(front, swapped, own)
        for i in range(out_ref.shape[0] // SEG):
            s = first + i
            rows = slice(s * SEG, (s + 1) * SEG)
            outs = slice(i * SEG, (i + 1) * SEG)
            query_map = feature(q_ref[rows, cols]).astype(BF)
            mem = before[:DH]
            norm = before[DH : DH + 1] + norm_ref[h, s : s + 1, :]
            if s > 0:
                mem = mem + inner_ref[s - 1, h]
            norm = jnp.broadcast_to(norm.astype(BF), (DH, DH))
            top = jnp.dot(query_map, mem.astype(BF), preferred_element_type=F32)
            bottom = lax.dot_general(query_map, norm, (((1,), (1,)), ((), ())), preferred_element_type=F32)
            recall = gate_ref[h : h + 1, :] * (top / (bottom + 1.0))
            out_ref[outs, cols] = (recall + local_ref[rows, cols].astype(F32)).astype(BF)


def most_kernel(at_ref, own_ref, prev_ref, next_ref, w_ref, out_ref, *far_refs):
    width = own_ref.shape[1]
    groups = w_ref.shape[0] // width
    tile = w_ref.shape[1] // 4
    for j in range(4):
        cols = slice(j * tile, (j + 1) * tile)

        def part(offset):
            start = pl.multiple_of(lax.rem(at_ref[0] + offset, groups) * width, width)
            return w_ref[pl.ds(start, width), cols]

        acc = jnp.dot(own_ref[...], part(0), preferred_element_type=F32)
        acc = acc + jnp.dot(prev_ref[...], part(groups - 1), preferred_element_type=F32)
        out_ref[:, cols] = acc + jnp.dot(next_ref[...], part(1), preferred_element_type=F32)
        for far_ref in far_refs:
            far_ref[:, cols] = part(2)


def rest_kernel(first, most_ref, far_a_ref, far_b_ref, w_ref, *refs):
    out_ref, done_ref, sems = refs[-3:]
    rows, n = done_ref.shape
    tile = n // 4
    far = jnp.concatenate([far_a_ref[...], far_b_ref[...]], axis=0)
    copies = []
    for j in range(4):
        cols = pl.ds(j * tile, tile)
        acc = most_ref[:, cols] + jnp.dot(far, w_ref[:, cols], preferred_element_type=F32)
        done_ref[:, cols] = acc.astype(done_ref.dtype)
        copy = pltpu.make_async_copy(done_ref.at[:, cols], out_ref.at[pl.ds(first, rows), cols], sems.at[j])
        copy.start()
        copies.append(copy)
    for copy in copies:
        copy.wait()


VMEM_SPEC = pl.BlockSpec(memory_space=pltpu.VMEM)
SMEM_SPEC = pl.BlockSpec(memory_space=pltpu.SMEM)


def near_core(x):
    return pltpu.with_memory_space_constraint(x, pltpu.VMEM)


def params(mib):
    return pltpu.CompilerParams(vmem_limit_bytes=mib * 2**20)


HBM_SPEC = pl.BlockSpec(memory_space=pltpu.HBM)


def far_core(x):
    return pltpu.with_memory_space_constraint(x, pltpu.HBM)


def state_call(keys, values):
    heads = keys.shape[1] // DH
    segs = keys.shape[0] // SEG
    return pl.pallas_call(
        state_kernel,
        in_specs=[HBM_SPEC] * 2,
        out_specs=(VMEM_SPEC,) * 3,
        out_shape=(
            pltpu.VMEM((heads, ROWS, DH), F32),
            pltpu.VMEM((segs - 1, heads, DH, DH), F32),
            pltpu.VMEM((heads, 8, DH), F32),
        ),
        scratch_shapes=[pltpu.VMEM(keys.shape, BF)] * 2 + [pltpu.SemaphoreType.DMA((2 * segs,))],
        compiler_params=params(4),
        name="state",
    )(far_core(keys), far_core(values))


def local_call(gate, q, k, v):
    n, width = q.shape
    return pl.pallas_call(
        local_kernel,
        in_specs=[VMEM_SPEC] + [HBM_SPEC] * 3,
        out_specs=VMEM_SPEC,
        out_shape=pltpu.VMEM((n, width), BF),
        scratch_shapes=[pltpu.VMEM(q.shape, BF)] * 3 + [pltpu.SemaphoreType.DMA((3 * n // SEG,))],
        compiler_params=params(6),
        cost_estimate=pl.CostEstimate(
            flops=4 * n * SEG * width, transcendentals=n * SEG * 4, bytes_accessed=8 * n * width
        ),
        name="local",
    )(gate, *map(far_core, (q, k, v)))


def context_call(first, count, gate, q, local, own, swapped, inner, norm):
    return pl.pallas_call(
        lambda *refs: context_kernel(first, *refs),
        in_specs=[VMEM_SPEC] * 7,
        out_specs=VMEM_SPEC,
        out_shape=pltpu.VMEM((count * SEG, q.shape[1]), BF),
        compiler_params=params(3),
        cost_estimate=pl.CostEstimate(
            flops=4 * count * SEG * q.shape[1] * DH, transcendentals=0, bytes_accessed=6 * count * SEG * q.shape[1]
        ),
    )(gate, q, local, near_core(own), near_core(swapped), inner, norm)


def most_call(at, own, prev, nxt, weight, far_rows):
    rows, n = own.shape[0], weight.shape[1]
    return pl.pallas_call(
        most_kernel,
        in_specs=[SMEM_SPEC] + [VMEM_SPEC] * 4,
        out_specs=(VMEM_SPEC,) * (1 + far_rows),
        out_shape=(pltpu.VMEM((rows, n), F32),) + (pltpu.VMEM((own.shape[1], n), BF),) * far_rows,
        compiler_params=params(4),
        cost_estimate=pl.CostEstimate(
            flops=2 * rows * weight.shape[0] * n, transcendentals=0, bytes_accessed=2 * weight.shape[0] * n
        ),
    )(at, own, near_core(prev), near_core(nxt), weight)


def rest_call(most, far_a, far_b, weight, total_rows, first, so_far):
    rows, n = most.shape
    operands = [most, near_core(far_a), near_core(far_b), weight]
    specs = [VMEM_SPEC] * 4
    aliases = {}
    if so_far is not None:
        aliases = {len(operands): 0}
        operands.append(so_far)
        specs.append(pl.BlockSpec(memory_space=pl.ANY))
    return pl.pallas_call(
        lambda *refs: rest_kernel(first, *refs),
        in_specs=specs,
        out_specs=pl.BlockSpec(memory_space=pl.ANY),
        out_shape=jax.ShapeDtypeStruct((total_rows, n), BF),
        scratch_shapes=[pltpu.VMEM((rows, n), BF), pltpu.SemaphoreType.DMA((4,))],
        input_output_aliases=aliases,
        compiler_params=params(4),
        cost_estimate=pl.CostEstimate(
            flops=2 * rows * far_a.shape[1] * n, transcendentals=0, bytes_accessed=8 * rows * n
        ),
    )(*operands)


def ring(size, step):
    return [(i, (i + step) % size) for i in range(size)]


def turn(value, axis, step):
    return lax.ppermute(value, axis, ring(lax.axis_size(axis), step))


def plane_kernel(at_ref, mine_ref, got_ref, *refs):
    *piece_refs, plane_ref, sent_ref, before_ref = refs
    x = at_ref[1:2, :]
    plane = mine_ref[...] + got_ref[...].astype(F32)
    before = jnp.zeros_like(plane)
    for k, ref in enumerate(piece_refs):
        piece = ref[...].astype(F32)
        plane = plane + piece
        before = before + jnp.where(x > k, piece, 0.0)
    plane_ref[...] = plane
    sent_ref[...] = plane.astype(BF)
    before_ref[...] = before


def window_kernel(size, at_ref, plane_ref, below_ref, above_ref, in_ref, window_ref, distant_ref, before_ref):
    z = at_ref[2:3, :]
    below = below_ref[...].astype(F32)
    above = above_ref[...].astype(F32)
    window = plane_ref[...] + jnp.where(z > 0.0, below, 0.0) + jnp.where(z < size - 1.0, above, 0.0)
    window_ref[...] = window.astype(BF)
    distant_ref[...] = jnp.where(z == size - 1.0, above, window).astype(BF)
    before_ref[...] = in_ref[...] + jnp.where(z == 1.0, below, 0.0) + jnp.where(z == size - 1.0, above, 0.0)


def before_kernel(at_ref, in_ref, lower_ref, upper_ref, mine_ref, got_ref, own_ref, sent_ref):
    first = at_ref[0:1, :] == 0.0
    z = at_ref[2:3, :]
    before = in_ref[...] + jnp.where(z >= 4.0, lower_ref[...].astype(F32), 0.0)
    before = before + jnp.where(z >= 2.0, upper_ref[...].astype(F32), 0.0)
    sent_ref[...] = jnp.where(first, before + mine_ref[...], before).astype(BF)
    own_ref[...] = jnp.where(first, before, before + got_ref[...].astype(F32))


def glue_call(kernel, at, arrays, dtypes):
    return pl.pallas_call(
        kernel,
        in_specs=[VMEM_SPEC] * (1 + len(arrays)),
        out_specs=(VMEM_SPEC,) * len(dtypes),
        out_shape=tuple(pltpu.VMEM(arrays[0].shape, dtype) for dtype in dtypes),
        compiler_params=params(2),
    )(at, *map(near_core, arrays))


def states_before(total, at):
    heads = total.shape[0]
    halves = total.reshape(2, heads // 2 * ROWS, DH)
    core = lax.axis_index("seq_2")
    mine = lax.dynamic_index_in_dim(halves, core, 0, keepdims=False)
    theirs = lax.dynamic_index_in_dim(halves, 1 - core, 0, keepdims=False)
    got = lax.ppermute(theirs.astype(BF), "seq_2", ring(2, 1))
    sent = (mine + got.astype(F32)).astype(BF)
    size = lax.axis_size("seq_1")
    pieces = [lax.ppermute(sent, "seq_1", ring(size, k)) for k in range(1, size)]
    plane, sent, before = glue_call(plane_kernel, at, (mine, got, *pieces), (F32, BF, F32))
    size = lax.axis_size("seq_0")
    below = lax.ppermute(sent, "seq_0", ring(size, 1))
    above = lax.ppermute(sent, "seq_0", ring(size, -1))
    window, distant, before = glue_call(
        lambda *refs: window_kernel(size, *refs), at, (plane, below, above, before), (BF, BF, F32)
    )
    lower = lax.ppermute(distant, "seq_0", [(0, 5), (1, 6), (2, 7), (7, 4)])
    upper = lax.ppermute(window, "seq_0", [(i, i + 2) for i in range(size - 2)])
    own, sent = glue_call(before_kernel, at, (before, lower, upper, mine, got), (F32, BF))
    return own, lax.ppermute(sent, "seq_2", ring(2, 1))


def layer(queries, keys, values, gate_bias, out_weight):
    rows = queries.shape[0]
    spans = ((0, 2), (2, 2))
    near_at = jnp.stack([lax.axis_index(axis).astype(F32) for axis in reversed(SEQ)])
    near_at = jnp.pad(jnp.broadcast_to(near_at[:, None], (3, DH)), ((0, 5), (0, 0)))
    gate = jnp.broadcast_to(jax.nn.sigmoid(gate_bias)[:, None], (gate_bias.shape[0], DH))
    gate = near_core(jnp.concatenate([gate, near_at[:4]], axis=0))
    near_at = near_core(near_at)
    at = jnp.full((1,), lax.axis_index("head"), jnp.int32)
    total, inner, norm = state_call(keys, values)
    own_before, swapped_before = states_before(total, near_at)
    near_q = near_core(queries)
    local = local_call(gate, queries, keys, values)
    weight = near_core(out_weight)
    out = far_weight = None
    pieces = []
    for c, (first, count) in enumerate(spans):
        own = context_call(first, count, gate, near_q, local, own_before, swapped_before, inner, norm)
        half = own.shape[0] // 2
        prev = turn(own, "head", 1)
        nxt = turn(own, "head", -1)
        far_a = turn(prev[:half], "head", 1)
        far_b = turn(nxt[half:], "head", -1)
        most, *extra = most_call(at, own, prev, nxt, weight, c == 1)
        far_weight = extra[0] if extra else far_weight
        pieces.append((most, far_a, far_b))
    for c, (first, count) in enumerate(spans):
        out = rest_call(*pieces[c], far_weight, rows, first * SEG, out)
    return out


def solution(mesh):
    finer = Mesh(
        mesh.devices.reshape(8, 4, 2, mesh.shape["head"]), ("seq_0", "seq_1", "seq_2", "head")
    )
    placed = (P(SEQ, "head"), P(SEQ, "head"), P(SEQ, "head"), P("head"), P(None, "head"))
    return jax.shard_map(layer, mesh=finer, in_specs=placed, out_specs=P(SEQ, "head"), check_vma=False)
```

```python
import jax
import jax.numpy as jnp
from jax import lax
from jax.experimental import pallas as pl
from jax.experimental.pallas import tpu as pltpu
from jax.sharding import Mesh
from jax.sharding import PartitionSpec as P

DH = 128
SEG = 256
SEQ = ("seq_0", "seq_1", "seq_2")
BF = jnp.bfloat16
F32 = jnp.float32
ROWS = DH + 8


def feature(x):
    x = x.astype(F32)
    return jnp.where(x > 0.0, x + 1.0, jnp.exp(jnp.minimum(x, 0.0)))


def fetch(start, sources, targets, sems):
    segs = targets[0].shape[0] // SEG
    copies = []
    for s in range(segs):
        rows = pl.ds(s * SEG, SEG)
        taken = pl.ds(start + s * SEG, SEG)
        group = []
        for i, (source, target) in enumerate(zip(sources, targets)):
            copy = pltpu.make_async_copy(source.at[taken], target.at[rows], sems.at[s * len(sources) + i])
            copy.start()
            group.append(copy)
        copies.append(group)
    return copies


def own_half(heads):
    return lax.axis_index("seq_2") * (heads // 2)


def state_kernel(bias_hbm, k_hbm, v_hbm, total_ref, inner_ref, norm_ref, gate_ref, k_ref, v_ref, bias_ref, sems):
    segs = k_ref.shape[0] // SEG
    heads = k_ref.shape[1] // DH
    first = own_half(heads)
    copies = fetch(0, (k_hbm, v_hbm), (k_ref, v_ref), sems)
    bias_copy = pltpu.make_async_copy(bias_hbm, bias_ref, sems.at[2 * segs])
    bias_copy.start()
    norms = [jnp.zeros((ROWS - DH, DH), F32)] * heads
    for s in range(segs):
        rows = slice(s * SEG, (s + 1) * SEG)
        for copy in copies[s]:
            copy.wait()
        for h in range(heads):
            cols = pl.ds(pl.multiple_of(lax.rem(first + h, heads) * DH, DH), DH)
            norm_ref[h, s : s + 1, :] = norms[h][:1]
            key_map = feature(k_ref[rows, cols]).astype(BF)
            mem = lax.dot_general(
                key_map, v_ref[rows, cols], (((0,), (0,)), ((), ())), preferred_element_type=F32
            )
            if s > 0:
                mem = mem + inner_ref[s - 1, h]
            norms[h] = norms[h] + jnp.dot(jnp.ones((ROWS - DH, SEG), BF), key_map, preferred_element_type=F32)
            if s < segs - 1:
                inner_ref[s, h] = mem
            else:
                total_ref[h, :DH, :] = mem
                total_ref[h, DH:, :] = norms[h]
    bias_copy.wait()
    for h in range(heads):
        bias = jnp.full((1, DH), bias_ref[lax.rem(first + h, heads)], F32)
        gate_ref[h : h + 1, :] = 1.0 / (1.0 + jnp.exp(-bias))


def local_kernel(start, gate_ref, q_hbm, k_hbm, v_hbm, out_ref, map_ref, q_ref, k_ref, v_ref, sems):
    heads = q_ref.shape[1] // DH
    first = own_half(heads)
    scale = 1.0 / DH**0.5 * 1.4426950408889634
    copies = fetch(start, (q_hbm, k_hbm, v_hbm), (q_ref, k_ref, v_ref), sems)
    for s in range(q_ref.shape[0] // SEG):
        rows = slice(s * SEG, (s + 1) * SEG)
        for copy in copies[s]:
            copy.wait()
        for h in range(heads):
            half, at = divmod(h, heads // 2)
            outs = slice(at * DH, (at + 1) * DH)
            cols = pl.ds(pl.multiple_of(lax.rem(first + h, heads) * DH, DH), DH)
            rest = 1.0 - gate_ref[h : h + 1, :]
            query = q_ref[rows, cols]
            map_ref[half, rows, outs] = feature(query).astype(BF)
            scores = lax.dot_general(
                query, k_ref[rows, cols], (((1,), (1,)), ((), ())), preferred_element_type=F32
            )
            row_at = lax.broadcasted_iota(jnp.int32, (SEG, SEG), 0)
            col_at = lax.broadcasted_iota(jnp.int32, (SEG, SEG), 1)
            scores = jnp.where(row_at >= col_at, scores * scale, -1e30)
            weights = jnp.exp2(scores - jnp.max(scores, axis=1, keepdims=True)).astype(BF)
            wide = jnp.concatenate([v_ref[rows, cols], jnp.ones((SEG, DH), BF)], axis=1)
            out = jnp.dot(weights, wide, preferred_element_type=F32)
            out_ref[half, rows, outs] = (out[:, :DH] * (rest / out[:, DH:])).astype(out_ref.dtype)


def context_kernel(half, gate_ref, before_ref, inner_ref, norm_ref, *refs):
    out_ref = refs[-1]
    parts = (len(refs) - 1) // 2
    count = out_ref.shape[1] // DH
    for i in range(count):
        h = half * count + i
        cols = slice(i * DH, (i + 1) * DH)
        before = before_ref[i * ROWS : i * ROWS + DH, :].astype(F32)
        norm_before = before_ref[i * ROWS + DH : i * ROWS + DH + 1, :].astype(F32)
        for s in range(out_ref.shape[0] // SEG):
            local_ref, map_ref = refs[s * parts * SEG // out_ref.shape[0] * 2 :][:2]
            at = s * SEG % map_ref.shape[1]
            query_map = map_ref[half, at : at + SEG, cols]
            mem = before
            norm = norm_before + norm_ref[h, s : s + 1, :]
            if s > 0:
                mem = mem + inner_ref[s - 1, h]
            norm = jnp.broadcast_to(norm.astype(BF), (DH, DH))
            top = jnp.dot(query_map, mem.astype(BF), preferred_element_type=F32)
            bottom = lax.dot_general(query_map, norm, (((1,), (1,)), ((), ())), preferred_element_type=F32)
            recall = gate_ref[h : h + 1, :] * (top / (bottom + 1.0))
            local = local_ref[half, at : at + SEG, cols].astype(F32)
            out_ref[s * SEG : (s + 1) * SEG, cols] = (recall + local).astype(BF)


def weight_part(w_ref, half, offset, width, cols):
    groups = w_ref.shape[0] // (2 * width)
    group = lax.rem(lax.axis_index("head") + offset, groups)
    core = lax.axis_index("seq_2")
    part = core if half == 0 else 1 - core
    return w_ref[pl.ds(pl.multiple_of((group * 2 + part) * width, width), width), cols]


def most_kernel(half, own_ref, prev_ref, next_ref, w_ref, *refs):
    out_ref = refs[-1]
    _, width = own_ref.shape
    tile = w_ref.shape[1] // 4
    for j in range(4):
        cols = slice(j * tile, (j + 1) * tile)
        acc = jnp.dot(own_ref[...], weight_part(w_ref, half, 0, width, cols), preferred_element_type=F32)
        acc = acc + jnp.dot(prev_ref[...], weight_part(w_ref, half, 3, width, cols), preferred_element_type=F32)
        acc = acc + jnp.dot(next_ref[...], weight_part(w_ref, half, 1, width, cols), preferred_element_type=F32)
        if len(refs) > 1:
            sum_ref, far_a_ref, far_b_ref = refs[:3]
            far = jnp.concatenate([far_a_ref[...], far_b_ref[...]], axis=0)
            acc = acc + jnp.dot(far, weight_part(w_ref, 0, 2, width, cols), preferred_element_type=F32)
            acc = acc + sum_ref[:, cols]
        out_ref[:, cols] = acc


def rest_kernel(most_ref, far_a_ref, far_b_ref, w_ref, out_ref, done_ref, sems):
    _, n = done_ref.shape
    half, width = far_a_ref.shape
    tile = n // 4
    copies = []
    for i, far_ref in enumerate((far_a_ref, far_b_ref)):
        outs = pl.ds(i * half, half)
        for j in range(4):
            cols = pl.ds(j * tile, tile)
            acc = jnp.dot(far_ref[...], weight_part(w_ref, 1, 2, width, cols), preferred_element_type=F32)
            done_ref[outs, cols] = (most_ref[outs, cols] + acc).astype(done_ref.dtype)
            copy = pltpu.make_async_copy(done_ref.at[outs, cols], out_ref.at[outs, cols], sems.at[i * 4 + j])
            copy.start()
            copies.append(copy)
    for copy in copies:
        copy.wait()


VMEM_SPEC = pl.BlockSpec(memory_space=pltpu.VMEM)


def near_core(x):
    return pltpu.with_memory_space_constraint(x, pltpu.VMEM)


def params(mib):
    return pltpu.CompilerParams(vmem_limit_bytes=mib * 2**20)


HBM_SPEC = pl.BlockSpec(memory_space=pltpu.HBM)


def far_core(x):
    return pltpu.with_memory_space_constraint(x, pltpu.HBM)


def state_call(bias, keys, values):
    heads = keys.shape[1] // DH
    segs = keys.shape[0] // SEG
    return pl.pallas_call(
        state_kernel,
        in_specs=[HBM_SPEC] * 3,
        out_specs=(VMEM_SPEC,) * 4,
        out_shape=(
            pltpu.VMEM((heads, ROWS, DH), F32),
            pltpu.VMEM((segs - 1, heads, DH, DH), F32),
            pltpu.VMEM((heads, 8, DH), F32),
            pltpu.VMEM((8, DH), F32),
        ),
        scratch_shapes=[pltpu.VMEM(keys.shape, BF)] * 2
        + [pltpu.SMEM(bias.shape, F32), pltpu.SemaphoreType.DMA((2 * segs + 1,))],
        compiler_params=params(4),
        name="state",
    )(*map(far_core, (bias, keys, values)))


def local_call(gate, q, k, v, start, count):
    width = q.shape[1]
    shape = (2, count, width // 2)
    return pl.pallas_call(
        lambda *refs: local_kernel(start, *refs),
        in_specs=[VMEM_SPEC] + [HBM_SPEC] * 3,
        out_specs=(VMEM_SPEC,) * 2,
        out_shape=(pltpu.VMEM(shape, BF),) * 2,
        scratch_shapes=[pltpu.VMEM((count, width), BF)] * 3 + [pltpu.SemaphoreType.DMA((3 * count // SEG,))],
        compiler_params=params(5),
        cost_estimate=pl.CostEstimate(
            flops=4 * count * SEG * width, transcendentals=count * SEG * 4, bytes_accessed=8 * count * width
        ),
    )(gate, *map(far_core, (q, k, v)))


def context_call(half, gate, before, inner, norm, parts):
    rows = sum(part[0].shape[1] for part in parts)
    width = parts[0][0].shape[2]
    flat = [x for part in parts for x in part]
    return pl.pallas_call(
        lambda *refs: context_kernel(half, *refs),
        in_specs=[VMEM_SPEC] * (4 + len(flat)),
        out_specs=VMEM_SPEC,
        out_shape=pltpu.VMEM((rows, width), BF),
        compiler_params=params(3),
        cost_estimate=pl.CostEstimate(
            flops=4 * rows * width * DH, transcendentals=0, bytes_accessed=6 * rows * width
        ),
    )(gate, near_core(before), inner, norm, *flat)


def most_call(half, own, prev, nxt, weight, *more):
    rows, n = own.shape[0], weight.shape[1]
    operands = [own, near_core(prev), near_core(nxt), weight, *(near_core(x) for x in more)]
    return pl.pallas_call(
        lambda *refs: most_kernel(half, *refs),
        in_specs=[VMEM_SPEC] * len(operands),
        out_specs=VMEM_SPEC,
        out_shape=pltpu.VMEM((rows, n), F32),
        compiler_params=params(4),
        cost_estimate=pl.CostEstimate(
            flops=2 * rows * weight.shape[0] * n // 2, transcendentals=0, bytes_accessed=2 * weight.shape[0] * n
        ),
    )(*operands)


def rest_call(most, far_a, far_b, weight):
    rows, n = most.shape
    return pl.pallas_call(
        rest_kernel,
        in_specs=[VMEM_SPEC] * 4,
        out_specs=pl.BlockSpec(memory_space=pl.ANY),
        out_shape=jax.ShapeDtypeStruct((rows, n), BF),
        scratch_shapes=[pltpu.VMEM((rows, n), BF), pltpu.SemaphoreType.DMA((8,))],
        compiler_params=params(4),
        cost_estimate=pl.CostEstimate(
            flops=2 * rows * far_a.shape[1] * n, transcendentals=0, bytes_accessed=8 * rows * n
        ),
        name="rest",
    )(near_core(most), near_core(far_a), near_core(far_b), weight)


def ring(size, step):
    return [(i, (i + step) % size) for i in range(size)]


def turn(value, axis, step):
    return lax.ppermute(value, axis, ring(lax.axis_size(axis), step))


def plane_kernel(mine_ref, got_ref, *refs):
    *piece_refs, plane_ref, sent_ref, before_ref = refs
    x = lax.axis_index("seq_1")
    plane = mine_ref[...] + got_ref[...].astype(F32)
    before = jnp.zeros_like(plane)
    for k, ref in enumerate(piece_refs):
        piece = ref[...].astype(F32)
        plane = plane + piece
        before = before + jnp.where(x > k, piece, 0.0)
    plane_ref[...] = plane
    sent_ref[...] = plane.astype(BF)
    before_ref[...] = before


def window_kernel(plane_ref, below_ref, above_ref, in_ref, window_ref, distant_ref, before_ref):
    z = lax.axis_index("seq_0")
    last = lax.axis_size("seq_0") - 1
    below = below_ref[...].astype(F32)
    above = above_ref[...].astype(F32)
    window = plane_ref[...] + jnp.where(z > 0, below, 0.0) + jnp.where(z < last, above, 0.0)
    window_ref[...] = window.astype(BF)
    distant_ref[...] = jnp.where(z == last, above, window).astype(BF)
    before_ref[...] = in_ref[...] + jnp.where(z == 1, below, 0.0) + jnp.where(z == last, above, 0.0)


def before_kernel(in_ref, lower_ref, upper_ref, mine_ref, got_ref, own_ref, sent_ref):
    first = lax.axis_index("seq_2") == 0
    z = lax.axis_index("seq_0")
    before = in_ref[...] + jnp.where(z >= 4, lower_ref[...].astype(F32), 0.0)
    before = before + jnp.where(z >= 2, upper_ref[...].astype(F32), 0.0)
    sent_ref[...] = jnp.where(first, before + mine_ref[...], before).astype(BF)
    own_ref[...] = jnp.where(first, before, before + got_ref[...].astype(F32))


def glue_call(kernel, arrays, dtypes):
    return pl.pallas_call(
        kernel,
        in_specs=[VMEM_SPEC] * len(arrays),
        out_specs=(VMEM_SPEC,) * len(dtypes),
        out_shape=tuple(pltpu.VMEM(arrays[0].shape, dtype) for dtype in dtypes),
        compiler_params=params(2),
    )(*map(near_core, arrays))


def states_before(total):
    heads = total.shape[0]
    halves = total.reshape(2, heads // 2 * ROWS, DH)
    mine, theirs = halves[0], halves[1]
    got = lax.ppermute(theirs.astype(BF), "seq_2", ring(2, 1))
    sent = (mine + got.astype(F32)).astype(BF)
    size = lax.axis_size("seq_1")
    pieces = [lax.ppermute(sent, "seq_1", ring(size, k)) for k in range(1, size)]
    plane, sent, before = glue_call(plane_kernel, (mine, got, *pieces), (F32, BF, F32))
    size = lax.axis_size("seq_0")
    below = lax.ppermute(sent, "seq_0", ring(size, 1))
    above = lax.ppermute(sent, "seq_0", ring(size, -1))
    window, distant, before = glue_call(window_kernel, (plane, below, above, before), (BF, BF, F32))
    upper = lax.ppermute(window, "seq_0", [(i, i + 2) for i in range(size - 2)])
    lower = lax.ppermute(distant, "seq_0", [(0, 5), (1, 6), (2, 7), (7, 4)])
    own, sent = glue_call(before_kernel, (before, lower, upper, mine, got), (F32, BF))
    return own, lax.ppermute(sent, "seq_2", ring(2, 1))


def layer(queries, keys, values, gate_bias, out_weight):
    rows = queries.shape[0]
    total, inner, norm, gate = state_call(gate_bias, keys, values)
    befores = states_before(total)
    parts = []
    for i in range(2):
        parts.append(local_call(gate, queries, keys, values, i * rows // 2, rows // 2))
    weight = near_core(out_weight)
    pieces = []
    for c in range(2):
        own = context_call(c, gate, befores[c], inner, norm, parts)
        prev = turn(own, "head", 1)
        nxt = turn(own, "head", -1)
        far_a = turn(prev[: rows // 2], "head", 1)
        far_b = turn(nxt[rows // 2 :], "head", -1)
        pieces.append((own, prev, nxt, far_a, far_b))
    most = most_call(0, *pieces[0][:3], weight)
    most = most_call(1, *pieces[1][:3], weight, most, *pieces[0][3:])
    return rest_call(most, *pieces[1][3:], weight)


def solution(mesh):
    finer = Mesh(
        mesh.devices.reshape(8, 4, 2, mesh.shape["head"]), ("seq_0", "seq_1", "seq_2", "head")
    )
    placed = (P(SEQ, "head"), P(SEQ, "head"), P(SEQ, "head"), P("head"), P(None, "head"))
    return jax.shard_map(layer, mesh=finer, in_specs=placed, out_specs=P(SEQ, "head"), check_vma=False)
```

```python
import jax
import jax.numpy as jnp
from jax import lax
from jax.experimental import pallas as pl
from jax.experimental.pallas import tpu as pltpu
from jax.sharding import Mesh
from jax.sharding import PartitionSpec as P

DH = 128
SEG = 256
SEQ = ("seq_0", "seq_1", "seq_2")
BF = jnp.bfloat16
F32 = jnp.float32
ROWS = DH + 8


def feature(x):
    x = x.astype(F32)
    return jnp.where(x > 0.0, x + 1.0, jnp.exp(jnp.minimum(x, 0.0)))


def fetch(start, sources, targets, sems):
    segs = targets[0].shape[0] // SEG
    copies = []
    for s in range(segs):
        rows = pl.ds(s * SEG, SEG)
        taken = pl.ds(start + s * SEG, SEG)
        group = []
        for i, (source, target) in enumerate(zip(sources, targets)):
            copy = pltpu.make_async_copy(source.at[taken], target.at[rows], sems.at[s * len(sources) + i])
            copy.start()
            group.append(copy)
        copies.append(group)
    return copies


def own_half(heads):
    return lax.axis_index("seq_2") * (heads // 2)


def add_states(first, count, k_ref, v_ref, s, last, norms, refs):
    total_ref, inner_ref, norm_ref = refs
    rows = slice(s * SEG, (s + 1) * SEG)
    for h in range(count):
        cols = pl.ds(first(h), DH)
        norm_ref[h, s : s + 1, :] = norms[h][:1]
        key_map = feature(k_ref[rows, cols]).astype(BF)
        mem = lax.dot_general(
            key_map, v_ref[rows, cols], (((0,), (0,)), ((), ())), preferred_element_type=F32
        )
        if s > 0:
            mem = mem + inner_ref[s - 1, h]
        norms[h] = norms[h] + jnp.dot(jnp.ones((ROWS - DH, SEG), BF), key_map, preferred_element_type=F32)
        if not last:
            inner_ref[s, h] = mem
        else:
            total_ref[h * ROWS : h * ROWS + DH, :] = mem.astype(total_ref.dtype)
            total_ref[h * ROWS + DH : (h + 1) * ROWS, :] = norms[h].astype(total_ref.dtype)


def other_state_kernel(bias_hbm, k_hbm, v_hbm, total_ref, inner_ref, norm_ref, gate_ref, kv_ref, k_ref, v_ref, bias_ref, sems):
    segs = k_ref.shape[0] // SEG
    heads = 2 * k_ref.shape[1] // DH
    width = k_ref.shape[1]
    mine = pl.multiple_of(lax.axis_index("seq_2") * width, width)
    theirs = pl.multiple_of((1 - lax.axis_index("seq_2")) * width, width)
    copies = fetch(0, (k_hbm.at[:, pl.ds(theirs, width)], v_hbm.at[:, pl.ds(theirs, width)]), (k_ref, v_ref), sems)
    extra = [
        pltpu.make_async_copy(bias_hbm, bias_ref, sems.at[2 * segs]),
        pltpu.make_async_copy(k_hbm.at[:, pl.ds(mine, width)], kv_ref.at[0], sems.at[2 * segs + 1]),
        pltpu.make_async_copy(v_hbm.at[:, pl.ds(mine, width)], kv_ref.at[1], sems.at[2 * segs + 2]),
    ]
    for copy in extra:
        copy.start()
    norms = [jnp.zeros((ROWS - DH, DH), F32)] * (heads // 2)
    for s in range(segs):
        for copy in copies[s]:
            copy.wait()
        add_states(lambda h: h * DH, heads // 2, k_ref, v_ref, s, s == segs - 1, norms, (total_ref, inner_ref, norm_ref))
    for copy in extra:
        copy.wait()
    for h in range(heads):
        bias = jnp.full((1, DH), bias_ref[lax.rem(own_half(heads) + h, heads)], F32)
        gate_ref[h : h + 1, :] = 1.0 / (1.0 + jnp.exp(-bias))


def own_state_kernel(kv_ref, total_ref, inner_ref, norm_ref):
    segs = kv_ref.shape[1] // SEG
    count = kv_ref.shape[2] // DH
    norms = [jnp.zeros((ROWS - DH, DH), F32)] * count
    for s in range(segs):
        add_states(
            lambda h: h * DH, count, kv_ref.at[0], kv_ref.at[1], s, s == segs - 1, norms, (total_ref, inner_ref, norm_ref)
        )


def local_kernel(gate_ref, *refs):
    ahead = len(refs) > 4
    if ahead:
        q_hbm, k_hbm, v_hbm, out_ref, map_ref, next_ref, q_ref, k_ref, v_ref, sems = refs
        count = q_ref.shape[0]
        copies = fetch(0, (q_hbm, k_hbm, v_hbm), (q_ref, k_ref, v_ref), sems)
        more = [
            pltpu.make_async_copy(ref.at[pl.ds(count, count)], next_ref.at[i], sems.at[3 * count // SEG + i])
            for i, ref in enumerate((q_hbm, k_hbm, v_hbm))
        ]
        for copy in more:
            copy.start()
    else:
        next_ref, out_ref, map_ref = refs
        q_ref, k_ref, v_ref = (next_ref.at[i] for i in range(3))
    heads = q_ref.shape[1] // DH
    first = own_half(heads)
    scale = 1.0 / DH**0.5 * 1.4426950408889634
    for s in range(q_ref.shape[0] // SEG):
        rows = slice(s * SEG, (s + 1) * SEG)
        if ahead:
            for copy in copies[s]:
                copy.wait()
        for h in range(heads):
            half, at = divmod(h, heads // 2)
            outs = slice(at * DH, (at + 1) * DH)
            cols = pl.ds(pl.multiple_of(lax.rem(first + h, heads) * DH, DH), DH)
            rest = 1.0 - gate_ref[h : h + 1, :]
            query = q_ref[rows, cols]
            map_ref[half, rows, outs] = feature(query).astype(BF)
            scores = lax.dot_general(
                query, k_ref[rows, cols], (((1,), (1,)), ((), ())), preferred_element_type=F32
            )
            row_at = lax.broadcasted_iota(jnp.int32, (SEG, SEG), 0)
            col_at = lax.broadcasted_iota(jnp.int32, (SEG, SEG), 1)
            scores = jnp.where(row_at >= col_at, scores * scale, -1e30)
            weights = jnp.exp2(scores - jnp.max(scores, axis=1, keepdims=True)).astype(BF)
            wide = jnp.concatenate([v_ref[rows, cols], jnp.ones((SEG, DH), BF)], axis=1)
            out = jnp.dot(weights, wide, preferred_element_type=F32)
            out_ref[half, rows, outs] = (out[:, :DH] * (rest / out[:, DH:])).astype(out_ref.dtype)
    if ahead:
        for copy in more:
            copy.wait()


def context_kernel(half, gate_ref, before_ref, inner_ref, norm_ref, *refs):
    out_ref = refs[-1]
    parts = (len(refs) - 1) // 2
    count = out_ref.shape[1] // DH
    for i in range(count):
        h = half * count + i
        cols = slice(i * DH, (i + 1) * DH)
        before = before_ref[i * ROWS : i * ROWS + DH, :].astype(F32)
        norm_before = before_ref[i * ROWS + DH : i * ROWS + DH + 1, :].astype(F32)
        for s in range(out_ref.shape[0] // SEG):
            local_ref, map_ref = refs[s * parts * SEG // out_ref.shape[0] * 2 :][:2]
            at = s * SEG % map_ref.shape[1]
            query_map = map_ref[half, at : at + SEG, cols]
            mem = before
            norm = norm_before + norm_ref[i, s : s + 1, :]
            if s > 0:
                mem = mem + inner_ref[s - 1, i]
            norm = jnp.broadcast_to(norm.astype(BF), (DH, DH))
            top = jnp.dot(query_map, mem.astype(BF), preferred_element_type=F32)
            bottom = lax.dot_general(query_map, norm, (((1,), (1,)), ((), ())), preferred_element_type=F32)
            recall = gate_ref[h : h + 1, :] * (top / (bottom + 1.0))
            local = local_ref[half, at : at + SEG, cols].astype(F32)
            out_ref[s * SEG : (s + 1) * SEG, cols] = (recall + local).astype(BF)


def weight_part(w_ref, half, offset, width, cols):
    groups = w_ref.shape[0] // (2 * width)
    group = lax.rem(lax.axis_index("head") + offset, groups)
    core = lax.axis_index("seq_2")
    part = core if half == 0 else 1 - core
    return w_ref[pl.ds(pl.multiple_of((group * 2 + part) * width, width), width), cols]


def most_kernel(half, own_ref, prev_ref, next_ref, w_ref, *refs):
    out_ref = refs[-1]
    _, width = own_ref.shape
    tile = w_ref.shape[1] // 4
    for j in range(4):
        cols = slice(j * tile, (j + 1) * tile)
        acc = jnp.dot(own_ref[...], weight_part(w_ref, half, 0, width, cols), preferred_element_type=F32)
        acc = acc + jnp.dot(prev_ref[...], weight_part(w_ref, half, 3, width, cols), preferred_element_type=F32)
        acc = acc + jnp.dot(next_ref[...], weight_part(w_ref, half, 1, width, cols), preferred_element_type=F32)
        if len(refs) > 1:
            sum_ref, far_a_ref, far_b_ref = refs[:3]
            far = jnp.concatenate([far_a_ref[...], far_b_ref[...]], axis=0)
            acc = acc + jnp.dot(far, weight_part(w_ref, 0, 2, width, cols), preferred_element_type=F32)
            acc = acc + sum_ref[:, cols]
        out_ref[:, cols] = acc


def rest_kernel(most_ref, far_a_ref, far_b_ref, w_ref, out_ref, done_ref, sems):
    _, n = done_ref.shape
    half, width = far_a_ref.shape
    tile = n // 4
    copies = []
    for i, far_ref in enumerate((far_a_ref, far_b_ref)):
        outs = pl.ds(i * half, half)
        for j in range(4):
            cols = pl.ds(j * tile, tile)
            acc = jnp.dot(far_ref[...], weight_part(w_ref, 1, 2, width, cols), preferred_element_type=F32)
            done_ref[outs, cols] = (most_ref[outs, cols] + acc).astype(done_ref.dtype)
            copy = pltpu.make_async_copy(done_ref.at[outs, cols], out_ref.at[outs, cols], sems.at[i * 4 + j])
            copy.start()
            copies.append(copy)
    for copy in copies:
        copy.wait()


VMEM_SPEC = pl.BlockSpec(memory_space=pltpu.VMEM)


def near_core(x):
    return pltpu.with_memory_space_constraint(x, pltpu.VMEM)


def params(mib):
    return pltpu.CompilerParams(vmem_limit_bytes=mib * 2**20)


HBM_SPEC = pl.BlockSpec(memory_space=pltpu.HBM)


def far_core(x):
    return pltpu.with_memory_space_constraint(x, pltpu.HBM)


def state_calls(bias, keys, values):
    rows, width = keys.shape
    half = width // 2
    count = half // DH
    segs = rows // SEG
    shapes = (pltpu.VMEM((segs - 1, count, DH, DH), F32), pltpu.VMEM((count, 8, DH), F32))
    theirs, *other, gate, kv = pl.pallas_call(
        other_state_kernel,
        in_specs=[HBM_SPEC] * 3,
        out_specs=(VMEM_SPEC,) * 5,
        out_shape=(
            pltpu.VMEM((count * ROWS, DH), BF),
            *shapes,
            pltpu.VMEM((8, DH), F32),
            pltpu.VMEM((2, rows, half), BF),
        ),
        scratch_shapes=[pltpu.VMEM((rows, half), BF)] * 2
        + [pltpu.SMEM(bias.shape, F32), pltpu.SemaphoreType.DMA((2 * segs + 3,))],
        compiler_params=params(4),
        name="other_state",
    )(*map(far_core, (bias, keys, values)))
    mine, *own = pl.pallas_call(
        own_state_kernel,
        in_specs=[VMEM_SPEC],
        out_specs=(VMEM_SPEC,) * 3,
        out_shape=(pltpu.VMEM((count * ROWS, DH), F32), *shapes),
        compiler_params=params(4),
        name="own_state",
    )(kv)
    return mine, theirs, (own, other), gate


def local_call(gate, operands, count, ahead):
    width = operands[0].shape[-1]
    shape = (2, count, width // 2)
    out_shape = (pltpu.VMEM(shape, BF),) * 2
    scratch = []
    if ahead:
        out_shape += (pltpu.VMEM((3, count, width), BF),)
        scratch = [pltpu.VMEM((count, width), BF)] * 3 + [pltpu.SemaphoreType.DMA((3 * count // SEG + 3,))]
        operands = tuple(map(far_core, operands))
    return pl.pallas_call(
        local_kernel,
        in_specs=[VMEM_SPEC] + [HBM_SPEC if ahead else VMEM_SPEC] * len(operands),
        out_specs=(VMEM_SPEC,) * len(out_shape),
        out_shape=out_shape,
        scratch_shapes=scratch,
        compiler_params=params(5),
        cost_estimate=pl.CostEstimate(
            flops=4 * count * SEG * width, transcendentals=count * SEG * 4, bytes_accessed=8 * count * width
        ),
    )(gate, *operands)


def context_call(half, gate, before, inner, norm, parts):
    rows = sum(part[0].shape[1] for part in parts)
    width = parts[0][0].shape[2]
    flat = [x for part in parts for x in part]
    return pl.pallas_call(
        lambda *refs: context_kernel(half, *refs),
        in_specs=[VMEM_SPEC] * (4 + len(flat)),
        out_specs=VMEM_SPEC,
        out_shape=pltpu.VMEM((rows, width), BF),
        compiler_params=params(3),
        cost_estimate=pl.CostEstimate(
            flops=4 * rows * width * DH, transcendentals=0, bytes_accessed=6 * rows * width
        ),
    )(gate, near_core(before), inner, norm, *flat)


def most_call(half, own, prev, nxt, weight, *more):
    rows, n = own.shape[0], weight.shape[1]
    operands = [own, near_core(prev), near_core(nxt), weight, *(near_core(x) for x in more)]
    return pl.pallas_call(
        lambda *refs: most_kernel(half, *refs),
        in_specs=[VMEM_SPEC] * len(operands),
        out_specs=VMEM_SPEC,
        out_shape=pltpu.VMEM((rows, n), F32),
        compiler_params=params(4),
        cost_estimate=pl.CostEstimate(
            flops=2 * rows * weight.shape[0] * n // 2, transcendentals=0, bytes_accessed=2 * weight.shape[0] * n
        ),
    )(*operands)


def rest_call(most, far_a, far_b, weight):
    rows, n = most.shape
    return pl.pallas_call(
        rest_kernel,
        in_specs=[VMEM_SPEC] * 4,
        out_specs=pl.BlockSpec(memory_space=pl.ANY),
        out_shape=jax.ShapeDtypeStruct((rows, n), BF),
        scratch_shapes=[pltpu.VMEM((rows, n), BF), pltpu.SemaphoreType.DMA((8,))],
        compiler_params=params(4),
        cost_estimate=pl.CostEstimate(
            flops=2 * rows * far_a.shape[1] * n, transcendentals=0, bytes_accessed=8 * rows * n
        ),
        name="rest",
    )(near_core(most), near_core(far_a), near_core(far_b), weight)


def ring(size, step):
    return [(i, (i + step) % size) for i in range(size)]


def turn(value, axis, step):
    return lax.ppermute(value, axis, ring(lax.axis_size(axis), step))


def plane_kernel(mine_ref, got_ref, *refs):
    *piece_refs, plane_ref, sent_ref, before_ref = refs
    x = lax.axis_index("seq_1")
    plane = mine_ref[...] + got_ref[...].astype(F32)
    before = jnp.zeros_like(plane)
    for k, ref in enumerate(piece_refs):
        piece = ref[...].astype(F32)
        plane = plane + piece
        before = before + jnp.where(x > k, piece, 0.0)
    plane_ref[...] = plane
    sent_ref[...] = plane.astype(BF)
    before_ref[...] = before


def window_kernel(plane_ref, below_ref, above_ref, in_ref, window_ref, distant_ref, before_ref):
    z = lax.axis_index("seq_0")
    last = lax.axis_size("seq_0") - 1
    below = below_ref[...].astype(F32)
    above = above_ref[...].astype(F32)
    window = plane_ref[...] + jnp.where(z > 0, below, 0.0) + jnp.where(z < last, above, 0.0)
    window_ref[...] = window.astype(BF)
    distant_ref[...] = jnp.where(z == last, above, window).astype(BF)
    before_ref[...] = in_ref[...] + jnp.where(z == 1, below, 0.0) + jnp.where(z == last, above, 0.0)


def before_kernel(in_ref, lower_ref, upper_ref, mine_ref, got_ref, own_ref, sent_ref):
    first = lax.axis_index("seq_2") == 0
    z = lax.axis_index("seq_0")
    before = in_ref[...] + jnp.where(z >= 4, lower_ref[...].astype(F32), 0.0)
    before = before + jnp.where(z >= 2, upper_ref[...].astype(F32), 0.0)
    sent_ref[...] = jnp.where(first, before + mine_ref[...], before).astype(BF)
    own_ref[...] = jnp.where(first, before, before + got_ref[...].astype(F32))


def glue_call(kernel, arrays, dtypes):
    return pl.pallas_call(
        kernel,
        in_specs=[VMEM_SPEC] * len(arrays),
        out_specs=(VMEM_SPEC,) * len(dtypes),
        out_shape=tuple(pltpu.VMEM(arrays[0].shape, dtype) for dtype in dtypes),
        compiler_params=params(2),
    )(*map(near_core, arrays))


def states_before(mine, theirs):
    got = lax.ppermute(theirs, "seq_2", ring(2, 1))
    sent = (mine + got.astype(F32)).astype(BF)
    size = lax.axis_size("seq_1")
    pieces = [lax.ppermute(sent, "seq_1", ring(size, k)) for k in range(1, size)]
    plane, sent, before = glue_call(plane_kernel, (mine, got, *pieces), (F32, BF, F32))
    size = lax.axis_size("seq_0")
    below = lax.ppermute(sent, "seq_0", ring(size, 1))
    above = lax.ppermute(sent, "seq_0", ring(size, -1))
    window, distant, before = glue_call(window_kernel, (plane, below, above, before), (BF, BF, F32))
    upper = lax.ppermute(window, "seq_0", [(i, i + 2) for i in range(size - 2)])
    lower = lax.ppermute(distant, "seq_0", [(0, 5), (1, 6), (2, 7), (7, 4)])
    own, sent = glue_call(before_kernel, (before, lower, upper, mine, got), (F32, BF))
    return own, lax.ppermute(sent, "seq_2", ring(2, 1))


def layer(queries, keys, values, gate_bias, out_weight):
    rows = queries.shape[0]
    mine, theirs, inners, gate = state_calls(gate_bias, keys, values)
    befores = states_before(mine, theirs)
    *part, ahead = local_call(gate, (queries, keys, values), rows // 2, True)
    parts = [part, local_call(gate, (ahead,), rows // 2, False)]
    weight = near_core(out_weight)
    pieces = []
    for c in range(2):
        own = context_call(c, gate, befores[c], *inners[c], parts)
        prev = turn(own, "head", 1)
        nxt = turn(own, "head", -1)
        far_a = turn(prev[: rows // 2], "head", 1)
        far_b = turn(nxt[rows // 2 :], "head", -1)
        pieces.append((own, prev, nxt, far_a, far_b))
    most = most_call(0, *pieces[0][:3], weight)
    most = most_call(1, *pieces[1][:3], weight, most, *pieces[0][3:])
    return rest_call(most, *pieces[1][3:], weight)


def solution(mesh):
    finer = Mesh(
        mesh.devices.reshape(8, 4, 2, mesh.shape["head"]), ("seq_0", "seq_1", "seq_2", "head")
    )
    placed = (P(SEQ, "head"), P(SEQ, "head"), P(SEQ, "head"), P("head"), P(None, "head"))
    return jax.shard_map(layer, mesh=finer, in_specs=placed, out_specs=P(SEQ, "head"), check_vma=False)
```
